32 devices in a mesh: traj: 16 (over z, y, core), tm: 2 (over x).
Axes of the slice: x: 2, y: 2, z: 4, core: 2. Of those that a mesh axis runs over, the one named last changes fastest.
Arguments:
- states: float32 [2, 32, 4096], P('tm', None, 'traj'), may hold values from -6 to 6
- vectors: bfloat16 [64, 4096], P(None, 'traj'), may hold values from -6 to 6
- kernel_scale: float32 [2], P('tm'), may hold values from 6 to 16
- neighbour_blocks: int32 [32, 24], P('traj'), may hold values from 0 to 31, as said below
- neighbour_count: int32 [32], P('traj'), may hold values from 6 to 24, as said below
Outputs:
- result: float32 [64, 4096], P(None, 'traj')
The draws below stay inside these ranges and needn't reach their ends.
Inputs may be any that keep to these rules, and one draw needn't show every extreme that they name: `neighbour_blocks`: row b names 24 different blocks, the first of them b itself. Only the first neighbour_count[b] entries of row b of neighbour_blocks are neighbours of block b; some block uses all 24.
All inputs are finite; a program needn't handle non-finite values.
Results may differ from the reference program's by a relative error of at most 0.0013.
Values may be sent and summed in bfloat16 or wider, within the bound.
No kernel may reach another device: no remote copies, remote signals or barrier semaphores. Data moves between devices by JAX's collectives and lax.ppermute only.
A program may use at most 64 MiB of HBM per device.

```python
import math
import jax
import jax.numpy as jnp
from jax import lax

COORD = 32
VECS = 64
BLK = 128
NBR = 24
SLICES = 2
TRAJ_ALL = 4096
BLOCKS = 32


def draw_neighbour_blocks(key, part):
    keys = jax.random.split(jax.random.fold_in(key, 11), BLOCKS)

    def one_row(row_key):
        return jax.random.permutation(row_key, BLOCKS - 1)[:NBR - 1].astype(jnp.int32) + 1
    offsets = jax.vmap(one_row)(keys)
    owners = jnp.arange(BLOCKS, dtype=jnp.int32)[:, None]
    others = (owners + offsets) % BLOCKS
    return jnp.concatenate([owners, others], axis=1).astype(jnp.int32)


def draw_neighbour_count(key, part):
    lowest = max(NBR // 4, 1)
    spread = NBR - lowest
    raw = jax.random.randint(jax.random.fold_in(key, 12), (BLOCKS,), 0, spread + 1)
    counts = lowest + raw * raw * raw // max(spread * spread, 1)
    chosen = jax.random.randint(jax.random.fold_in(key, 13), (), 0, BLOCKS)
    counts = counts.at[chosen].set(NBR)
    return counts.astype(jnp.int32)


def steps_of(own_key, extent, cuts, least, high):
    level, own = 1.0, jax.random.fold_in(own_key, 6)
    for position, parts in cuts:
        steps = jnp.exp(jax.random.uniform(jax.random.fold_in(own, position), (parts,), jnp.float32, least / len(cuts), high / len(cuts)))
        level = level * jnp.repeat(steps, extent[position] // parts).reshape([-1 if axis == position else 1 for axis in range(len(extent))])
    return level


def bell_draw(key, dims, deviation, most, pieces=(), kind=jnp.bfloat16):
    entries = deviation * jax.random.normal(key, dims, jnp.float32)
    if pieces:
        entries = entries * steps_of(key, dims, pieces, -0.22, 0.18)
    return jnp.clip(entries, -most, most).astype(kind)


def setup_inputs(seed: int = 0) -> dict:
    key_of = jax.random.split(jax.random.key(seed), 6)
    return {
        "states": bell_draw(key_of[0], (SLICES, COORD, TRAJ_ALL), 1.0, 6.0, ((0, 2), (2, 16)), jnp.float32),
        "vectors": bell_draw(key_of[1], (VECS, TRAJ_ALL), 1.0, 6.0, ((1, 16),)),
        "kernel_scale": jnp.clip(jnp.exp(math.log(16.0) - 0.98082925 * jax.random.uniform(key_of[2], (SLICES,), jnp.float32) ** steps_of(key_of[2], (SLICES,), ((0, 2),), -0.2, 0.2)), 6.0, 16.0),
        "neighbour_blocks": draw_neighbour_blocks(jax.random.fold_in(key_of[5], 71), 0),
        "neighbour_count": draw_neighbour_count(jax.random.fold_in(key_of[5], 71), 0),
    }


def linked_blocks(neighbour_blocks, neighbour_count, blocks_total):
    slots = neighbour_blocks.shape[1]
    named = neighbour_blocks[:, :, None] == jnp.arange(blocks_total, dtype=jnp.int32)[None, None, :]
    within = jnp.arange(slots, dtype=jnp.int32)[None, :, None] < neighbour_count[:, None, None]
    return jnp.any(named & within, axis=1).astype(jnp.float32)


def reference(states, vectors, kernel_scale, neighbour_blocks, neighbour_count):
    columns = states.shape[2]
    blocks_total = columns // BLK
    linked = linked_blocks(neighbour_blocks, neighbour_count, blocks_total)

    def one_slice(running, slice_index):
        coords = states[slice_index]
        squares = jnp.sum(coords * coords, axis=0)
        spread = kernel_scale[slice_index]

        def one_block(running_block, block_index):
            row_start = (block_index * BLK).astype(jnp.int32)
            rows = lax.dynamic_slice_in_dim(coords, row_start, BLK, 1)
            cross = jnp.dot(rows.T, coords, precision=lax.Precision.HIGHEST)
            row_squares = lax.dynamic_slice_in_dim(squares, row_start, BLK, 0)
            distance = row_squares[:, None] + squares[None, :] - 2.0 * cross
            mask = jnp.repeat(linked[block_index], BLK)
            kernel = mask[None, :] * jnp.exp(-distance / spread)
            row_sum = jnp.sum(kernel, axis=1)
            weights = kernel.astype(jnp.bfloat16)
            pushed = lax.dot_general(vectors, weights, (((1,), (1,)), ((), ())), preferred_element_type=jnp.float32)
            scaled = (pushed / (row_sum * row_sum)[None, :]).astype(jnp.bfloat16)
            pulled = jnp.dot(scaled, weights, preferred_element_type=jnp.float32)
            return running_block + pulled, None

        running, unused = lax.scan(one_block, running, jnp.arange(blocks_total, dtype=jnp.int32))
        return running, None

    initial = jnp.zeros((vectors.shape[0], columns), jnp.float32)
    result, unused = lax.scan(one_slice, initial, jnp.arange(states.shape[0], dtype=jnp.int32))
    return result
```

```python
import functools
import math

import jax
import jax.numpy as jnp
from jax import lax
from jax.experimental import pallas as pl
from jax.experimental.pallas import tpu as pltpu
from jax.sharding import PartitionSpec as P

BLK = 128
AUX = 16
LINK_ROW = 6


VMEM = pl.BlockSpec(memory_space=pltpu.VMEM)
SMEM = pl.BlockSpec(memory_space=pltpu.SMEM)


def digits(n):
    out = []
    for radix in (2,):
        if n % radix == 0 and n > 1:
            out.append(radix)
            n //= radix
    if n % 4 == 0:
        mid = n // 4
        out += [r for r in (mid, 4) if r > 1]
    elif n > 1:
        out.append(n)
    return out


def staged_gather(x, n, axis):
    stages, stride = [], 1
    for radix in digits(n):
        stages.append((stride, radix))
        stride *= radix
    pieces = {0: x}
    for stride, radix in reversed(stages):
        fresh = {}
        for k in range(1, radix):
            hop = k * stride
            pairs = [(i, i ^ hop) for i in range(n)]
            for offset, piece in pieces.items():
                fresh[offset ^ hop] = lax.ppermute(piece, axis, pairs)
        pieces.update(fresh)
    return [pieces[o] for o in range(n)]


def split3(value):
    first = value.astype(jnp.bfloat16)
    rest = value - first.astype(jnp.float32)
    second = rest.astype(jnp.bfloat16)
    third = (rest - second.astype(jnp.float32)).astype(jnp.bfloat16)
    return [p.astype(jnp.float32) for p in (first, second, third)]


def prep_kernel(scale_ref, lists_ref, count_ref, states_ref, vectors_ref, msg_ref, left_ref):
    vecs = vectors_ref.shape[0]
    coords, rows = states_ref.shape[1], states_ref.shape[2]
    spread = jnp.full((1, rows), scale_ref[0], jnp.float32)
    factor = jnp.sqrt((2.0 * math.log2(math.e)) / spread)
    x = states_ref[0] * factor
    hi = x.astype(jnp.bfloat16).astype(jnp.float32)
    lo = (x - hi).astype(jnp.bfloat16).astype(jnp.float32)
    whole = hi + lo
    half = -0.5 * jnp.sum(whole * whole, axis=0, keepdims=True)
    pieces = split3(half)
    lane = lax.broadcasted_iota(jnp.int32, (1, rows), 1)
    linked = jnp.zeros((1, rows), jnp.float32)
    for h in range(rows // BLK):
        for slot in range(lists_ref.shape[1]):
            hit = (lane == lists_ref[h, slot] + h * BLK) & (slot < count_ref[h])
            linked = jnp.where(hit, 1.0, linked)
    sub = lax.broadcasted_iota(jnp.int32, (AUX, rows), 0)
    right = jnp.where((sub >= 3) & (sub < 6), 1.0, 0.0)
    left = jnp.where(sub < 3, 1.0, 0.0)
    for r, piece in enumerate(pieces):
        right = jnp.where(sub == r, piece, right)
        left = jnp.where(sub == r + 3, piece, left)
    right = jnp.where(sub == LINK_ROW, linked, right)
    msg_ref[0:vecs, :] = vectors_ref[...]
    msg_ref[vecs : vecs + coords, :] = hi.astype(jnp.bfloat16)
    msg_ref[vecs + coords : vecs + 2 * coords, :] = lo.astype(jnp.bfloat16)
    msg_ref[vecs + 2 * coords :, :] = right.astype(jnp.bfloat16)
    stacked = jnp.concatenate([hi, hi, left, lo, lo], axis=0)
    left_ref[...] = stacked.T.astype(jnp.bfloat16)


def push_kernel(n, vecs, me_ref, lists_ref, count_ref, left_ref, *refs):
    msgs, (scaled_ref, kern_ref, colm_ref, mask_ref, rows_ref) = refs[:n], refs[n:]
    rows = left_ref.shape[0]
    per = rows // BLK
    me = me_ref[0]
    for c in range(per):
        for g in range(n * per):
            mask_ref[c, g] = 0
        for slot in range(lists_ref.shape[1]):
            @pl.when(slot < count_ref[c])
            def _():
                mask_ref[c, lists_ref[c, slot]] = 1
    left = left_ref[...]
    sums = [jnp.zeros((BLK, BLK), jnp.float32) for _ in range(per)]
    pushed = [jnp.zeros((vecs, BLK), jnp.float32) for _ in range(per)]
    depth = left.shape[1] - AUX
    for o in range(n):
        feats = msgs[o][vecs:, :]
        right = jnp.concatenate([feats, msgs[o][vecs : vecs + depth // 2, :]], axis=0)
        arg = lax.dot_general(left, right, (((1,), (0,)), ((), ())), preferred_element_type=jnp.float32)
        kernel = jnp.exp2(arg)
        weights = kernel.astype(jnp.bfloat16)
        kern_ref[o] = weights
        vec = msgs[o][0:vecs, :]
        links = feats[depth // 2 + LINK_ROW : depth // 2 + LINK_ROW + 1, :].astype(jnp.float32)
        base = (me ^ o) * per
        for h in range(per):
            rows_ref[o * per + h : o * per + h + 1, :] = links[:, h * BLK : (h + 1) * BLK]
        for c in range(per):
            parts = []
            for h in range(per):
                m = mask_ref[c, base + h]
                cols = slice(h * BLK, (h + 1) * BLK)
                sums[c] = sums[c] + kernel[c * BLK : (c + 1) * BLK, cols] * m.astype(jnp.float32)
                parts.append(jnp.where(m > 0, vec[:, cols], jnp.zeros_like(vec[:, cols])))
            pushed[c] = pushed[c] + lax.dot_general(
                jnp.concatenate(parts, axis=1),
                weights[c * BLK : (c + 1) * BLK, :],
                (((1,), (1,)), ((), ())),
                preferred_element_type=jnp.float32,
            )
    for c in range(per):
        row_sum = jnp.sum(sums[c].T, axis=0, keepdims=True)
        scaled_ref[:, c * BLK : (c + 1) * BLK] = (pushed[c] / (row_sum * row_sum)).astype(jnp.bfloat16)
    table = rows_ref[...]
    lane = lax.broadcasted_iota(jnp.int32, table.shape, 1)
    for c in range(per):
        picked = jnp.sum(jnp.where(lane == me * per + c, table, 0.0), axis=1, keepdims=True)
        colm_ref[c] = jnp.broadcast_to(picked, table.shape)


def pull_kernel(n, colm_ref, kern_ref, *refs):
    pieces, out_ref = refs[:n], refs[n]
    vecs, rows = out_ref.shape
    per = rows // BLK
    total = [jnp.zeros((vecs, BLK), jnp.float32) for _ in range(per)]
    for o in range(n):
        piece = pieces[o][...]
        for c in range(per):
            parts = []
            for h in range(per):
                m = colm_ref[c, o * per + h : o * per + h + 1, :]
                part = piece[:, h * BLK : (h + 1) * BLK]
                parts.append(jnp.where(m > 0.5, part.astype(jnp.float32), 0.0).astype(jnp.bfloat16))
            total[c] = total[c] + lax.dot_general(
                jnp.concatenate(parts, axis=1),
                kern_ref[o, c * BLK : (c + 1) * BLK, :],
                (((1,), (1,)), ((), ())),
                preferred_element_type=jnp.float32,
            )
    for c in range(per):
        out_ref[:, c * BLK : (c + 1) * BLK] = total[c]


def per_device(n, slices, states, vectors, kernel_scale, neighbour_blocks, neighbour_count):
    coords, rows = states.shape[1], states.shape[2]
    vecs = vectors.shape[0]
    per = rows // BLK
    depth = 4 * coords + AUX
    me = lax.axis_index("traj").astype(jnp.int32).reshape(1)
    msg, left = pl.pallas_call(
        prep_kernel,
        out_shape=(
            jax.ShapeDtypeStruct((vecs + 2 * coords + AUX, rows), jnp.bfloat16),
            jax.ShapeDtypeStruct((rows, depth), jnp.bfloat16),
        ),
        in_specs=[SMEM, SMEM, SMEM, VMEM, VMEM],
        out_specs=(VMEM, VMEM),
        name="prep",
    )(kernel_scale, neighbour_blocks, neighbour_count, states, vectors)
    msgs = staged_gather(msg, n, "traj")
    scaled, kern, colm = pl.pallas_call(
        functools.partial(push_kernel, n, vecs),
        out_shape=(
            jax.ShapeDtypeStruct((vecs, rows), jnp.bfloat16),
            jax.ShapeDtypeStruct((n, rows, rows), jnp.bfloat16),
            jax.ShapeDtypeStruct((per, n * per, BLK), jnp.float32),
        ),
        in_specs=[SMEM, SMEM, SMEM, VMEM] + [VMEM] * n,
        out_specs=(VMEM, VMEM, VMEM),
        scratch_shapes=[pltpu.SMEM((per, n * per), jnp.int32), pltpu.VMEM((n * per, BLK), jnp.float32)],
        name="push",
    )(me, neighbour_blocks, neighbour_count, left, *msgs)
    pieces = staged_gather(scaled, n, "traj")
    total = pl.pallas_call(
        functools.partial(pull_kernel, n),
        out_shape=jax.ShapeDtypeStruct((vecs, rows), jnp.float32),
        in_specs=[VMEM, VMEM] + [VMEM] * n,
        out_specs=VMEM,
        name="pull",
    )(colm, kern, *pieces)
    hop = 1
    while hop < slices:
        total = total + lax.ppermute(total, "tm", [(i, i ^ hop) for i in range(slices)])
        hop *= 2
    return total


def solution(mesh):
    in_specs = (P("tm", None, "traj"), P(None, "traj"), P("tm"), P("traj", None), P("traj"))
    out_specs = P(None, "traj")
    return jax.shard_map(
        functools.partial(per_device, mesh.shape["traj"], mesh.shape["tm"]),
        mesh=mesh,
        in_specs=in_specs,
        out_specs=out_specs,
        check_vma=False,
    )
```

```python
import functools
import math

import jax
import jax.numpy as jnp
from jax import lax
from jax.experimental import pallas as pl
from jax.experimental.pallas import tpu as pltpu
from jax.sharding import PartitionSpec as P

BLK = 128
AUX = 16
LINK_ROW = 6


VMEM = pl.BlockSpec(memory_space=pltpu.VMEM)
SMEM = pl.BlockSpec(memory_space=pltpu.SMEM)
HBM = pl.BlockSpec(memory_space=pltpu.HBM)
PARAMS = pltpu.CompilerParams(vmem_limit_bytes=16 * 1024 * 1024)


def digits(n):
    out = []
    for radix in (2,):
        if n % radix == 0 and n > 1:
            out.append(radix)
            n //= radix
    if n % 4 == 0:
        mid = n // 4
        out += [r for r in (mid, 4) if r > 1]
    elif n > 1:
        out.append(n)
    return out


def staged_gather(x, n, axis):
    stages, stride = [], 1
    for radix in digits(n):
        stages.append((stride, radix))
        stride *= radix
    pieces = {0: x}
    for stride, radix in reversed(stages):
        fresh = {}
        for k in range(1, radix):
            hop = k * stride
            pairs = [(i, i ^ hop) for i in range(n)]
            for offset, piece in pieces.items():
                fresh[offset ^ hop] = lax.ppermute(piece, axis, pairs)
        pieces.update(fresh)
    return [pieces[o] for o in range(n)]


def split3(value):
    first = value.astype(jnp.bfloat16)
    rest = value - first.astype(jnp.float32)
    second = rest.astype(jnp.bfloat16)
    third = (rest - second.astype(jnp.float32)).astype(jnp.bfloat16)
    return [p.astype(jnp.float32) for p in (first, second, third)]


def prep_kernel(
    scale_ref, lists_hbm, count_hbm, states_hbm, vectors_hbm, msg_ref, left_ref,
    lists_ref, count_ref, states_ref, sems,
):
    vecs = vectors_hbm.shape[0]
    coords, rows = states_ref.shape[1], states_ref.shape[2]
    moves = [
        pltpu.make_async_copy(states_hbm, states_ref, sems.at[0]),
        pltpu.make_async_copy(lists_hbm, lists_ref, sems.at[1]),
        pltpu.make_async_copy(count_hbm, count_ref, sems.at[2]),
        pltpu.make_async_copy(vectors_hbm, msg_ref.at[0:vecs, :], sems.at[3]),
    ]
    for move in moves:
        move.start()
    for move in moves:
        move.wait()
    spread = jnp.full((1, rows), scale_ref[0], jnp.float32)
    factor = jnp.sqrt((2.0 * math.log2(math.e)) / spread)
    x = states_ref[0] * factor
    hi = x.astype(jnp.bfloat16).astype(jnp.float32)
    lo = (x - hi).astype(jnp.bfloat16).astype(jnp.float32)
    whole = hi + lo
    half = -0.5 * jnp.sum(whole * whole, axis=0, keepdims=True)
    pieces = split3(half)
    lane = lax.broadcasted_iota(jnp.int32, (1, rows), 1)
    linked = jnp.zeros((1, rows), jnp.float32)
    for h in range(rows // BLK):
        for slot in range(lists_ref.shape[1]):
            target = jnp.where(slot < count_ref[h], lists_ref[h, slot] + h * BLK, rows)
            linked = jnp.where(lane == target, 1.0, linked)
    sub = lax.broadcasted_iota(jnp.int32, (AUX, rows), 0)
    right = jnp.where((sub >= 3) & (sub < 6), 1.0, 0.0)
    left = jnp.where(sub < 3, 1.0, 0.0)
    for r, piece in enumerate(pieces):
        right = jnp.where(sub == r, piece, right)
        left = jnp.where(sub == r + 3, piece, left)
    right = jnp.where(sub == LINK_ROW, linked, right)
    msg_ref[vecs : vecs + coords, :] = hi.astype(jnp.bfloat16)
    msg_ref[vecs + coords : vecs + 2 * coords, :] = lo.astype(jnp.bfloat16)
    msg_ref[vecs + 2 * coords :, :] = right.astype(jnp.bfloat16)
    stacked = jnp.concatenate([hi, hi, left, lo, lo], axis=0)
    left_ref[...] = stacked.T.astype(jnp.bfloat16)


def push_kernel(n, vecs, me_ref, left_ref, *refs):
    msgs, (scaled_ref, kern_ref, colm_ref, rows_ref, mask_ref) = refs[:n], refs[n:]
    rows = left_ref.shape[0]
    per = rows // BLK
    me = me_ref[0]
    left = left_ref[...]
    depth = left.shape[1] - AUX
    for o in range(n):
        links = msgs[o][vecs + depth // 2 :, :].astype(jnp.float32)[LINK_ROW : LINK_ROW + 1, :]
        for h in range(per):
            rows_ref[o * per + h : o * per + h + 1, :] = links[:, h * BLK : (h + 1) * BLK]
    table = rows_ref[...]
    lane = lax.broadcasted_iota(jnp.int32, table.shape, 1)
    block = lax.broadcasted_iota(jnp.int32, table.shape, 0)
    block = ((block // per) ^ me) * per + block % per
    for c in range(per):
        picked = jnp.sum(jnp.where(lane == me * per + c, table, 0.0), axis=1, keepdims=True)
        colm_ref[c] = jnp.broadcast_to(picked, table.shape)
        picked = jnp.sum(jnp.where(lane == block, table[c : c + 1, :], 0.0), axis=1, keepdims=True)
        mask_ref[c] = jnp.broadcast_to(picked, table.shape)
    sums = [jnp.zeros((BLK, BLK), jnp.float32) for _ in range(per)]
    pushed = [jnp.zeros((vecs, BLK), jnp.float32) for _ in range(per)]
    for o in range(n):
        feats = msgs[o][vecs:, :]
        right = jnp.concatenate([feats, msgs[o][vecs : vecs + depth // 2, :]], axis=0)
        arg = lax.dot_general(left, right, (((1,), (0,)), ((), ())), preferred_element_type=jnp.float32)
        kernel = jnp.exp2(arg)
        weights = kernel.astype(jnp.bfloat16)
        kern_ref[o] = weights
        vec = msgs[o][0:vecs, :]
        for c in range(per):
            parts = []
            for h in range(per):
                m = mask_ref[c, o * per + h : o * per + h + 1, :]
                cols = slice(h * BLK, (h + 1) * BLK)
                sums[c] = sums[c] + kernel[c * BLK : (c + 1) * BLK, cols] * m
                parts.append(jnp.where(m > 0.5, vec[:, cols].astype(jnp.float32), 0.0).astype(jnp.bfloat16))
            pushed[c] = pushed[c] + lax.dot_general(
                jnp.concatenate(parts, axis=1),
                weights[c * BLK : (c + 1) * BLK, :],
                (((1,), (1,)), ((), ())),
                preferred_element_type=jnp.float32,
            )
    for c in range(per):
        row_sum = jnp.sum(sums[c].T, axis=0, keepdims=True)
        scaled_ref[:, c * BLK : (c + 1) * BLK] = (pushed[c] / (row_sum * row_sum)).astype(jnp.bfloat16)


def pull_kernel(n, colm_ref, kern_ref, *refs):
    pieces, out_ref = refs[:n], refs[n]
    vecs, rows = out_ref.shape
    per = rows // BLK
    total = [jnp.zeros((vecs, BLK), jnp.float32) for _ in range(per)]
    for o in range(n):
        piece = pieces[o][...]
        for c in range(per):
            parts = []
            for h in range(per):
                m = colm_ref[c, o * per + h : o * per + h + 1, :]
                part = piece[:, h * BLK : (h + 1) * BLK]
                parts.append(jnp.where(m > 0.5, part.astype(jnp.float32), 0.0).astype(jnp.bfloat16))
            total[c] = total[c] + lax.dot_general(
                jnp.concatenate(parts, axis=1),
                kern_ref[o, c * BLK : (c + 1) * BLK, :],
                (((1,), (1,)), ((), ())),
                preferred_element_type=jnp.float32,
            )
    for c in range(per):
        out_ref[:, c * BLK : (c + 1) * BLK] = total[c]


def in_hbm(*arrays):
    return [pltpu.with_memory_space_constraint(a, pltpu.HBM) for a in arrays]


def add_kernel(a_ref, b_ref, out_ref):
    out_ref[...] = a_ref[...] + b_ref[...]


def per_device(n, slices, states, vectors, kernel_scale, neighbour_blocks, neighbour_count):
    coords, rows = states.shape[1], states.shape[2]
    vecs = vectors.shape[0]
    per = rows // BLK
    depth = 4 * coords + AUX
    me = lax.axis_index("traj").astype(jnp.int32).reshape(1)
    msg, left = pl.pallas_call(
        prep_kernel,
        out_shape=(
            jax.ShapeDtypeStruct((vecs + 2 * coords + AUX, rows), jnp.bfloat16),
            jax.ShapeDtypeStruct((rows, depth), jnp.bfloat16),
        ),
        in_specs=[SMEM] + [HBM] * 4,
        out_specs=(VMEM, VMEM),
        scratch_shapes=[
            pltpu.SMEM(neighbour_blocks.shape, jnp.int32),
            pltpu.SMEM(neighbour_count.shape, jnp.int32),
            pltpu.VMEM(states.shape, jnp.float32),
            pltpu.SemaphoreType.DMA((4,)),
        ],
        compiler_params=PARAMS,
        name="prep",
    )(kernel_scale, *in_hbm(neighbour_blocks, neighbour_count, states, vectors))
    msgs = staged_gather(msg, n, "traj")
    scaled, kern, colm = pl.pallas_call(
        functools.partial(push_kernel, n, vecs),
        out_shape=(
            jax.ShapeDtypeStruct((vecs, rows), jnp.bfloat16),
            jax.ShapeDtypeStruct((n, rows, rows), jnp.bfloat16),
            jax.ShapeDtypeStruct((per, n * per, BLK), jnp.float32),
        ),
        in_specs=[SMEM, VMEM] + [VMEM] * n,
        out_specs=(VMEM, VMEM, VMEM),
        scratch_shapes=[pltpu.VMEM((n * per, BLK), jnp.float32), pltpu.VMEM((per, n * per, BLK), jnp.float32)],
        compiler_params=PARAMS,
        name="push",
    )(me, left, *msgs)
    pieces = staged_gather(scaled, n, "traj")
    total = pl.pallas_call(
        functools.partial(pull_kernel, n),
        out_shape=jax.ShapeDtypeStruct((vecs, rows), jnp.float32),
        in_specs=[VMEM, VMEM] + [VMEM] * n,
        out_specs=VMEM,
        compiler_params=PARAMS,
        name="pull",
    )(colm, kern, *pieces)
    hop = 1
    while hop < slices:
        other = lax.ppermute(total, "tm", [(i, i ^ hop) for i in range(slices)])
        total = pl.pallas_call(
            add_kernel,
            out_shape=jax.ShapeDtypeStruct((vecs, rows), jnp.float32),
            in_specs=[VMEM, VMEM],
            out_specs=VMEM,
            compiler_params=PARAMS,
            name="add",
        )(total, other)
        hop *= 2
    return total


def solution(mesh):
    in_specs = (P("tm", None, "traj"), P(None, "traj"), P("tm"), P("traj", None), P("traj"))
    out_specs = P(None, "traj")
    return jax.shard_map(
        functools.partial(per_device, mesh.shape["traj"], mesh.shape["tm"]),
        mesh=mesh,
        in_specs=in_specs,
        out_specs=out_specs,
        check_vma=False,
    )
```

```python
import functools
import math

import jax
import jax.numpy as jnp
from jax import lax
from jax.experimental import pallas as pl
from jax.experimental.pallas import tpu as pltpu
from jax.sharding import PartitionSpec as P

BLK = 128
AUX = 16
LINK_ROW = 6
LIST_ROW = 7
GROUP = 2
UNROLL = 16


VMEM = pl.BlockSpec(memory_space=pltpu.VMEM)
SMEM = pl.BlockSpec(memory_space=pltpu.SMEM)
HBM = pl.BlockSpec(memory_space=pltpu.HBM)
PARAMS = pltpu.CompilerParams(vmem_limit_bytes=16 * 1024 * 1024)


def digits(n):
    out = []
    for radix in (2,):
        if n % radix == 0 and n > 1:
            out.append(radix)
            n //= radix
    if n % 4 == 0:
        mid = n // 4
        out += [r for r in (mid, 4) if r > 1]
    elif n > 1:
        out.append(n)
    return out


def staged_gather(x, n, axis):
    stages, stride = [], 1
    for radix in digits(n):
        stages.append((stride, radix))
        stride *= radix
    pieces = {0: x}
    for stride, radix in reversed(stages):
        fresh = {}
        for k in range(1, radix):
            hop = k * stride
            pairs = [(i, i ^ hop) for i in range(n)]
            for offset, piece in pieces.items():
                fresh[offset ^ hop] = lax.ppermute(piece, axis, pairs)
        pieces.update(fresh)
    return [pieces[o] for o in range(n)]


def split3(value):
    first = value.astype(jnp.bfloat16)
    rest = value - first.astype(jnp.float32)
    second = rest.astype(jnp.bfloat16)
    third = (rest - second.astype(jnp.float32)).astype(jnp.bfloat16)
    return [p.astype(jnp.float32) for p in (first, second, third)]


def prep_kernel(
    blocks, scale_ref, lists_hbm, count_hbm, states_hbm, vectors_hbm, msg_ref, left_ref,
    lists_ref, count_ref, states_ref, sems,
):
    vecs = vectors_hbm.shape[0]
    coords, rows = states_ref.shape[1], states_ref.shape[2]
    moves = [
        pltpu.make_async_copy(states_hbm, states_ref, sems.at[0]),
        pltpu.make_async_copy(lists_hbm, lists_ref, sems.at[1]),
        pltpu.make_async_copy(count_hbm, count_ref, sems.at[2]),
        pltpu.make_async_copy(vectors_hbm, msg_ref.at[0:vecs, :], sems.at[3]),
    ]
    for move in moves:
        move.start()
    for move in moves:
        move.wait()
    spread = jnp.full((1, rows), scale_ref[0], jnp.float32)
    factor = jnp.sqrt((2.0 * math.log2(math.e)) / spread)
    x = states_ref[0] * factor
    hi = x.astype(jnp.bfloat16).astype(jnp.float32)
    lo = (x - hi).astype(jnp.bfloat16).astype(jnp.float32)
    whole = hi + lo
    half = -0.5 * jnp.sum(whole * whole, axis=0, keepdims=True)
    pieces = split3(half)
    lane = lax.broadcasted_iota(jnp.int32, (1, rows), 1)
    linked = jnp.zeros((1, rows), jnp.float32)
    listed = jnp.full((1, rows), blocks, jnp.int32)
    for h in range(rows // BLK):
        for slot in range(lists_ref.shape[1]):
            used = slot < count_ref[h]
            linked = jnp.where(lane == jnp.where(used, lists_ref[h, slot] + h * BLK, rows), 1.0, linked)
            listed = jnp.where(lane == slot + h * BLK, jnp.where(used, lists_ref[h, slot], blocks), listed)
        units = lax.shift_right_logical(count_ref[h] + (GROUP - 1), GROUP.bit_length() - 1)
        listed = jnp.where(lane == (h + 1) * BLK - 1, units, listed)
    sub = lax.broadcasted_iota(jnp.int32, (AUX, rows), 0)
    right = jnp.where((sub >= 3) & (sub < 6), 1.0, 0.0)
    left = jnp.where(sub < 3, 1.0, 0.0)
    for r, piece in enumerate(pieces):
        right = jnp.where(sub == r, piece, right)
        left = jnp.where(sub == r + 3, piece, left)
    right = jnp.where(sub == LINK_ROW, linked, right)
    right = jnp.where(sub == LIST_ROW, listed.astype(jnp.float32), right)
    msg_ref[vecs : vecs + coords, :] = hi.astype(jnp.bfloat16)
    msg_ref[vecs + coords : vecs + 2 * coords, :] = lo.astype(jnp.bfloat16)
    msg_ref[vecs + 2 * coords :, :] = right.astype(jnp.bfloat16)
    stacked = jnp.concatenate([hi, hi, left, lo, lo], axis=0)
    left_ref[...] = stacked.T.astype(jnp.bfloat16)


def left_kernel(half, vecs, *refs):
    msgs, (left_ref, lists_ref) = refs[:half], refs[half:]
    rows = msgs[0].shape[1]
    per = rows // BLK
    coords = (msgs[0].shape[0] - vecs - AUX) // 2
    sub = lax.broadcasted_iota(jnp.int32, (AUX, rows), 0)
    for m in range(half):
        hi = msgs[m][vecs : vecs + coords, :].astype(jnp.float32)
        lo = msgs[m][vecs + coords : vecs + 2 * coords, :].astype(jnp.float32)
        aux = msgs[m][vecs + 2 * coords :, :].astype(jnp.float32)
        left = jnp.where(sub < 3, 1.0, jnp.where(sub < 6, pltpu.roll(aux, 3, 0), 0.0))
        stacked = jnp.concatenate([hi, hi, left, lo, lo], axis=0).T.astype(jnp.bfloat16)
        for h in range(per):
            left_ref[m * per + h] = stacked[h * BLK : (h + 1) * BLK, :]
            row = aux[LIST_ROW : LIST_ROW + 1, h * BLK : (h + 1) * BLK]
            lists_ref[m * per + h : m * per + h + 1, :] = row.astype(jnp.int32)
    lists_ref[half * per :, :] = jnp.zeros((8, BLK), jnp.int32)
    left_ref[half * per] = jnp.zeros(left_ref.shape[1:], jnp.bfloat16)


def push_kernel(n, vecs, most, me_ref, lists_ref, left_ref, *refs):
    msgs, (scaled_ref, right_ref, vec_ref, sums_ref, pushed_ref, list_ref, unit_ref, sem) = refs[:n], refs[n:]
    rows = msgs[0].shape[1]
    per = rows // BLK
    feats = left_ref.shape[2] - AUX
    blocks = n * per
    tiles = n // 2 * per
    move = pltpu.make_async_copy(lists_ref, list_ref, sem)
    move.start()
    me = me_ref[0]
    for o in range(n):
        base = (me ^ o) * per
        for h in range(per):
            cols = slice(h * BLK, (h + 1) * BLK)
            part = msgs[o][vecs:, cols]
            right_ref[base + h] = jnp.concatenate([part, msgs[o][vecs : vecs + feats // 2, cols]], axis=0)
            vec_ref[base + h] = msgs[o][0:vecs, cols]
    sub = lax.broadcasted_iota(jnp.int32, right_ref.shape[1:], 0)
    right_ref[blocks] = jnp.where(sub == feats // 2, -3.0e4, 0.0).astype(jnp.bfloat16)
    vec_ref[blocks] = jnp.zeros(vec_ref.shape[1:], jnp.bfloat16)
    sums_ref[...] = jnp.zeros(sums_ref.shape, jnp.float32)
    pushed_ref[...] = jnp.zeros(pushed_ref.shape, jnp.float32)
    move.wait()
    start = 0
    for r in range(tiles):
        for k in range(most):
            unit_ref[start + k] = r * BLK + k * GROUP
        start = start + list_ref[r, BLK - 1]
    for k in range(UNROLL):
        unit_ref[start + k] = tiles * BLK

    def step(t, carry):
        for g in range(UNROLL):
            code = unit_ref[t * UNROLL + g]
            r = lax.shift_right_logical(code, 7)
            k = lax.bitwise_and(code, BLK - 1)
            ids = [list_ref[r, k + q] for q in range(GROUP)]
            right = jnp.concatenate([right_ref[b] for b in ids], axis=1)
            arg = lax.dot_general(left_ref[r], right, (((1,), (0,)), ((), ())), preferred_element_type=jnp.float32)
            kernel = jnp.exp2(arg)
            weights = kernel.astype(jnp.bfloat16)
            total = kernel[:, 0:BLK]
            for q in range(1, GROUP):
                total = total + kernel[:, q * BLK : (q + 1) * BLK]
            vec = jnp.concatenate([vec_ref[b] for b in ids], axis=1)
            push = lax.dot_general(vec, weights, (((1,), (1,)), ((), ())), preferred_element_type=jnp.float32)
            sums_ref[r] = sums_ref[r] + total
            pushed_ref[r] = pushed_ref[r] + push
        return carry

    lax.fori_loop(0, lax.shift_right_logical(start + (UNROLL - 1), UNROLL.bit_length() - 1), step, 0)
    for r in range(tiles):
        row_sum = jnp.sum(sums_ref[r].T, axis=0, keepdims=True)
        scaled_ref[:, r * BLK : (r + 1) * BLK] = (pushed_ref[r] / (row_sum * row_sum)).astype(jnp.bfloat16)


def pull_tile(piece, kernel, colm_ref, c, block):
    parts = []
    for h in range(piece.shape[1] // BLK):
        m = colm_ref[c, block + h : block + h + 1, :]
        part = piece[:, h * BLK : (h + 1) * BLK].astype(jnp.float32)
        parts.append(jnp.where(m > 0.5, part, 0.0).astype(jnp.bfloat16))
    return lax.dot_general(
        jnp.concatenate(parts, axis=1), kernel, (((1,), (1,)), ((), ())), preferred_element_type=jnp.float32
    )


def own_kernel(n, vecs, me_ref, left_ref, scaled_ref, *refs):
    msgs, (partial_ref, kern_ref, colm_ref, rows_ref) = refs[:n], refs[n:]
    rows = left_ref.shape[0]
    per = rows // BLK
    me = me_ref[0]
    left = left_ref[...]
    feats = left.shape[1] - AUX
    for o in range(n):
        links = msgs[o][vecs + feats // 2 :, :].astype(jnp.float32)[LINK_ROW : LINK_ROW + 1, :]
        for h in range(per):
            rows_ref[o * per + h : o * per + h + 1, :] = links[:, h * BLK : (h + 1) * BLK]
    table = rows_ref[...]
    lane = lax.broadcasted_iota(jnp.int32, table.shape, 1)
    for c in range(per):
        picked = jnp.sum(jnp.where(lane == me * per + c, table, 0.0), axis=1, keepdims=True)
        colm_ref[c] = jnp.broadcast_to(picked, table.shape)
    total = [jnp.zeros((vecs, BLK), jnp.float32) for _ in range(per)]
    for o in range(n):
        right = jnp.concatenate([msgs[o][vecs:, :], msgs[o][vecs : vecs + feats // 2, :]], axis=0)
        arg = lax.dot_general(left, right, (((1,), (0,)), ((), ())), preferred_element_type=jnp.float32)
        weights = jnp.exp2(arg).astype(jnp.bfloat16)
        if o % 2:
            kern_ref[o // 2] = weights
        else:
            piece = scaled_ref[:, o // 2 * rows : (o // 2 + 1) * rows]
            for c in range(per):
                total[c] = total[c] + pull_tile(piece, weights[c * BLK : (c + 1) * BLK, :], colm_ref, c, o * per)
    for c in range(per):
        partial_ref[:, c * BLK : (c + 1) * BLK] = total[c]


def pull_kernel(n, partial_ref, colm_ref, kern_ref, scaled_ref, out_ref):
    rows = out_ref.shape[1]
    per = rows // BLK
    for c in range(per):
        cols = slice(c * BLK, (c + 1) * BLK)
        total = partial_ref[:, cols]
        for m in range(n // 2):
            piece = scaled_ref[:, m * rows : (m + 1) * rows]
            total = total + pull_tile(piece, kern_ref[m, cols, :], colm_ref, c, (2 * m + 1) * per)
        out_ref[:, cols] = total


def in_hbm(*arrays):
    return [pltpu.with_memory_space_constraint(a, pltpu.HBM) for a in arrays]


def add_kernel(a_ref, b_ref, out_ref):
    out_ref[...] = a_ref[...] + b_ref[...]


def per_device(n, slices, states, vectors, kernel_scale, neighbour_blocks, neighbour_count):
    coords, rows = states.shape[1], states.shape[2]
    vecs = vectors.shape[0]
    per = rows // BLK
    depth = 4 * coords + AUX
    me = lax.axis_index("traj").astype(jnp.int32).reshape(1)
    msg, left = pl.pallas_call(
        functools.partial(prep_kernel, n * per),
        out_shape=(
            jax.ShapeDtypeStruct((vecs + 2 * coords + AUX, rows), jnp.bfloat16),
            jax.ShapeDtypeStruct((rows, depth), jnp.bfloat16),
        ),
        in_specs=[SMEM] + [HBM] * 4,
        out_specs=(VMEM, VMEM),
        scratch_shapes=[
            pltpu.SMEM(neighbour_blocks.shape, jnp.int32),
            pltpu.SMEM(neighbour_count.shape, jnp.int32),
            pltpu.VMEM(states.shape, jnp.float32),
            pltpu.SemaphoreType.DMA((4,)),
        ],
        compiler_params=PARAMS,
        name="prep",
    )(kernel_scale, *in_hbm(neighbour_blocks, neighbour_count, states, vectors))
    msgs = staged_gather(msg, n, "traj")
    half = n // 2
    tiles = half * per
    most = -(-neighbour_blocks.shape[1] // GROUP)
    lefts, lists = pl.pallas_call(
        functools.partial(left_kernel, half, vecs),
        out_shape=(
            jax.ShapeDtypeStruct((tiles + 1, BLK, depth), jnp.bfloat16),
            jax.ShapeDtypeStruct((tiles + 8, BLK), jnp.int32),
        ),
        in_specs=[VMEM] * half,
        out_specs=(VMEM, VMEM),
        compiler_params=PARAMS,
        name="left",
    )(*msgs[::2])
    scaled = pl.pallas_call(
        functools.partial(push_kernel, n, vecs, most),
        out_shape=jax.ShapeDtypeStruct((vecs, half * rows), jnp.bfloat16),
        in_specs=[SMEM, VMEM, VMEM] + [VMEM] * n,
        out_specs=VMEM,
        scratch_shapes=[
            pltpu.VMEM((n * per + 1, depth, BLK), jnp.bfloat16),
            pltpu.VMEM((n * per + 1, vecs, BLK), jnp.bfloat16),
            pltpu.VMEM((tiles + 1, BLK, BLK), jnp.float32),
            pltpu.VMEM((tiles + 1, vecs, BLK), jnp.float32),
            pltpu.SMEM((tiles + 8, BLK), jnp.int32),
            pltpu.SMEM((tiles * most + most + UNROLL,), jnp.int32),
            pltpu.SemaphoreType.DMA,
        ],
        compiler_params=PARAMS,
        name="push",
    )(me, lists, lefts, *msgs)
    across = lax.ppermute(scaled, "traj", [(i, i ^ 1) for i in range(n)])
    partial, kern, colm = pl.pallas_call(
        functools.partial(own_kernel, n, vecs),
        out_shape=(
            jax.ShapeDtypeStruct((vecs, rows), jnp.float32),
            jax.ShapeDtypeStruct((half, rows, rows), jnp.bfloat16),
            jax.ShapeDtypeStruct((per, n * per, BLK), jnp.float32),
        ),
        in_specs=[SMEM, VMEM, VMEM] + [VMEM] * n,
        out_specs=(VMEM, VMEM, VMEM),
        scratch_shapes=[pltpu.VMEM((n * per, BLK), jnp.float32)],
        compiler_params=PARAMS,
        cost_estimate=pl.CostEstimate(flops=2 * n * rows * rows * (depth + vecs), bytes_accessed=1 << 20, transcendentals=0),
        name="own",
    )(me, left, scaled, *msgs)
    total = pl.pallas_call(
        functools.partial(pull_kernel, n),
        out_shape=jax.ShapeDtypeStruct((vecs, rows), jnp.float32),
        in_specs=[VMEM] * 4,
        out_specs=VMEM,
        compiler_params=PARAMS,
        name="pull",
    )(partial, colm, kern, across)
    hop = 1
    while hop < slices:
        other = lax.ppermute(total, "tm", [(i, i ^ hop) for i in range(slices)])
        total = pl.pallas_call(
            add_kernel,
            out_shape=jax.ShapeDtypeStruct((vecs, rows), jnp.float32),
            in_specs=[VMEM, VMEM],
            out_specs=VMEM,
            compiler_params=PARAMS,
            name="add",
        )(total, other)
        hop *= 2
    return total


def solution(mesh):
    in_specs = (P("tm", None, "traj"), P(None, "traj"), P("tm"), P("traj", None), P("traj"))
    out_specs = P(None, "traj")
    return jax.shard_map(
        functools.partial(per_device, mesh.shape["traj"], mesh.shape["tm"]),
        mesh=mesh,
        in_specs=in_specs,
        out_specs=out_specs,
        check_vma=False,
    )
```

```python
import functools
import math

import jax
import jax.numpy as jnp
from jax import lax
from jax.experimental import pallas as pl
from jax.experimental.pallas import tpu as pltpu
from jax.sharding import PartitionSpec as P


BLK = 128
AUX = 8
LINK_ROW = 6
LIST_ROW = 7
GROUP = 2
COVER = 10000000
BIG = 52
SMALL = 16
ROUND = 27


VMEM = pl.BlockSpec(memory_space=pltpu.VMEM)
SMEM = pl.BlockSpec(memory_space=pltpu.SMEM)
HBM = pl.BlockSpec(memory_space=pltpu.HBM)
PARAMS = pltpu.CompilerParams(vmem_limit_bytes=16 * 1024 * 1024)


def plan(n):
    core = 2 if n % 2 == 0 else 1
    wide = 4 if n % (4 * core) == 0 else 1
    mid = n // (core * wide)
    stride = core * mid
    steps = []

    def middle(piece):
        return [(piece, k * core) for k in range(1, mid)]

    if wide == 4:
        steps += [(0, 2 * stride), (0, stride)] + middle(0) + [(2 * stride, stride)]
        steps += middle(2 * stride) + middle(stride) + middle(3 * stride)
    else:
        steps += middle(0)
    order = [0] + [piece ^ hop for piece, hop in steps]
    if core == 2:
        steps += [(piece, 1) for piece in order]
    return steps


def staged_gather(x, n, axis, tied):
    pieces = {0: x}
    for i, (piece, hop) in enumerate(plan(n)):
        if i == 1:
            pieces[0], tied = lax.optimization_barrier((pieces[0], tied))
        pieces[piece ^ hop] = lax.ppermute(pieces[piece], axis, [(d, d ^ hop) for d in range(n)])
    return [pieces[o] for o in range(n)], tied


def split3(value):
    first = value.astype(jnp.bfloat16)
    rest = value - first.astype(jnp.float32)
    second = rest.astype(jnp.bfloat16)
    third = (rest - second.astype(jnp.float32)).astype(jnp.bfloat16)
    return [p.astype(jnp.float32) for p in (first, second, third)]


def prep_kernel(blocks, lists_hbm, count_hbm, states_hbm, vectors_hbm, msg_ref, lists_ref, count_ref, states_ref, sems):
    vecs = vectors_hbm.shape[0]
    coords, rows = states_ref.shape[1], states_ref.shape[2]
    moves = [
        pltpu.make_async_copy(lists_hbm, lists_ref, sems.at[0]),
        pltpu.make_async_copy(count_hbm, count_ref, sems.at[1]),
        pltpu.make_async_copy(states_hbm, states_ref, sems.at[2]),
        pltpu.make_async_copy(vectors_hbm, msg_ref.at[0:vecs, :], sems.at[3]),
    ]
    for move in moves:
        move.start()
    for move in moves:
        move.wait()
    x = states_ref[0]
    hi = x.astype(jnp.bfloat16).astype(jnp.float32)
    lo = (x - hi).astype(jnp.bfloat16).astype(jnp.float32)
    whole = hi + lo
    pieces = split3(-0.5 * jnp.sum(whole * whole, axis=0, keepdims=True))
    lane = lax.broadcasted_iota(jnp.int32, (1, rows), 1)
    linked = jnp.zeros((1, rows), jnp.float32)
    listed = jnp.full((1, rows), blocks, jnp.int32)
    for h in range(rows // BLK):
        for slot in range(lists_ref.shape[1]):
            used = slot < count_ref[h]
            linked = jnp.where(lane == jnp.where(used, lists_ref[h, slot] + h * BLK, rows), 1.0, linked)
            listed = jnp.where(lane == slot + h * BLK, jnp.where(used, lists_ref[h, slot], blocks), listed)
        units = lax.shift_right_logical(count_ref[h] + (GROUP - 1), GROUP.bit_length() - 1)
        listed = jnp.where(lane == (h + 1) * BLK - 1, units, listed)
    sub = lax.broadcasted_iota(jnp.int32, (AUX, rows), 0)
    aux = jnp.where((sub >= 3) & (sub < 6), 1.0, 0.0)
    for r, piece in enumerate(pieces):
        aux = jnp.where(sub == r, piece, aux)
    aux = jnp.where(sub == LINK_ROW, linked, aux)
    aux = jnp.where(sub == LIST_ROW, listed.astype(jnp.float32), aux)
    msg_ref[vecs : vecs + coords, :] = hi.astype(jnp.bfloat16)
    msg_ref[vecs + coords : vecs + 2 * coords, :] = lo.astype(jnp.bfloat16)
    msg_ref[vecs + 2 * coords :, :] = aux.astype(jnp.bfloat16)


def factor_kernel(scale_ref, out_ref):
    out_ref[...] = (2.0 * math.log2(math.e)) / jnp.full(out_ref.shape, scale_ref[0], jnp.float32)


def right_side(msg, vecs, cols):
    feats = msg[vecs : msg.shape[0] - AUX, cols]
    return jnp.concatenate([feats, feats, msg[msg.shape[0] - AUX :, cols]], axis=0)


def stage_block(msg, vecs, base, right_ref, vec_ref):
    for h in range(msg.shape[1] // BLK):
        cols = slice(h * BLK, (h + 1) * BLK)
        right_ref[base + h] = right_side(msg, vecs, cols)
        vec_ref[base + h] = msg[0:vecs, cols]


def left_kernel(half, vecs, me_ref, *refs):
    msgs, (left_ref, lists_ref, right_ref, vec_ref, sums_ref, pushed_ref) = refs[:half], refs[half:]
    rows = msgs[0].shape[1]
    per = rows // BLK
    coords = (msgs[0].shape[0] - vecs - AUX) // 2
    blocks = 2 * half * per
    me = me_ref[0]
    sub = lax.broadcasted_iota(jnp.int32, (AUX, rows), 0)
    for m in range(half):
        hi = msgs[m][vecs : vecs + coords, :].astype(jnp.float32)
        lo = msgs[m][vecs + coords : vecs + 2 * coords, :].astype(jnp.float32)
        aux = msgs[m][vecs + 2 * coords :, :].astype(jnp.float32)
        left = jnp.where(sub < 3, 1.0, jnp.where(sub < 6, pltpu.roll(aux, 3, 0), 0.0))
        stacked = jnp.concatenate([hi, hi, lo, lo, left], axis=0).T.astype(jnp.bfloat16)
        for h in range(per):
            left_ref[m * per + h] = stacked[h * BLK : (h + 1) * BLK, :]
            row = aux[LIST_ROW : LIST_ROW + 1, h * BLK : (h + 1) * BLK]
            lists_ref[m * per + h : m * per + h + 1, :] = row.astype(jnp.int32)
        stage_block(msgs[m], vecs, (me ^ (2 * m)) * per, right_ref, vec_ref)
    lists_ref[half * per :, :] = jnp.zeros((8, BLK), jnp.int32)
    left_ref[half * per] = jnp.zeros(left_ref.shape[1:], jnp.bfloat16)
    sub = lax.broadcasted_iota(jnp.int32, right_ref.shape[1:], 0)
    right_ref[blocks] = jnp.where(sub == 4 * coords, -3.0e4, 0.0).astype(jnp.bfloat16)
    vec_ref[blocks] = jnp.zeros(vec_ref.shape[1:], jnp.bfloat16)
    sums_ref[...] = jnp.zeros(sums_ref.shape, jnp.float32)
    pushed_ref[...] = jnp.zeros(pushed_ref.shape, jnp.float32)


def push_kernel(half, vecs, most, me_ref, factor_ref, lists_ref, left_ref, *refs):
    msgs, refs = refs[:half], refs[half + 4 :]
    right_ref, vec_ref, sums_ref, pushed_ref, scaled_ref, list_ref, unit_ref, sem = refs
    per = msgs[0].shape[1] // BLK
    tiles = half * per
    move = pltpu.make_async_copy(lists_ref, list_ref, sem)
    move.start()
    me = me_ref[0]
    for m in range(half):
        stage_block(msgs[m], vecs, (me ^ (2 * m + 1)) * per, right_ref, vec_ref)
    factors = jnp.concatenate([factor_ref[0:1, :]] * GROUP, axis=1)
    move.wait()
    start = 0
    for r in range(tiles):
        for k in range(most):
            unit_ref[start + k] = r * BLK + k * GROUP
        start = start + list_ref[r, BLK - 1]
    for k in range(BIG):
        unit_ref[start + k] = tiles * BLK

    def visit(code):
        r = lax.shift_right_logical(code, 7)
        k = lax.bitwise_and(code, BLK - 1)
        ids = [list_ref[r, k + q] for q in range(GROUP)]
        right = jnp.concatenate([right_ref[b] for b in ids], axis=1)
        arg = lax.dot_general(left_ref[r], right, (((1,), (0,)), ((), ())), preferred_element_type=jnp.float32)
        kernel = jnp.exp2(arg * factors)
        weights = kernel.astype(jnp.bfloat16)
        total = kernel[:, 0:BLK]
        for q in range(1, GROUP):
            total = total + kernel[:, q * BLK : (q + 1) * BLK]
        vec = jnp.concatenate([vec_ref[b] for b in ids], axis=1)
        push = lax.dot_general(vec, weights, (((1,), (1,)), ((), ())), preferred_element_type=jnp.float32)
        sums_ref[r] = sums_ref[r] + total
        pushed_ref[r] = pushed_ref[r] + push

    def big_step(t, carry):
        for g in range(BIG):
            visit(unit_ref[t * BIG + g])
        return carry

    def small_step(t, first):
        for g in range(SMALL):
            visit(unit_ref[first + t * SMALL + g])
        return first

    bigs = lax.div(start + ROUND, BIG)
    rest = jnp.maximum(start - bigs * BIG, 0)
    lax.fori_loop(0, bigs, big_step, 0)
    lax.fori_loop(0, lax.div(rest + (SMALL - 1), SMALL), small_step, bigs * BIG)
    for r in range(tiles):
        row_sum = jnp.sum(sums_ref[r].T, axis=0, keepdims=True)
        scaled_ref[:, r * BLK : (r + 1) * BLK] = (pushed_ref[r] / (row_sum * row_sum)).astype(jnp.bfloat16)


def pull_tile(piece, kernel, colm_ref, c, block):
    parts = []
    for h in range(piece.shape[1] // BLK):
        m = colm_ref[c, block + h : block + h + 1, :]
        part = piece[:, h * BLK : (h + 1) * BLK].astype(jnp.float32)
        parts.append(jnp.where(m > 0.5, part, 0.0).astype(jnp.bfloat16))
    return lax.dot_general(
        jnp.concatenate(parts, axis=1), kernel, (((1,), (1,)), ((), ())), preferred_element_type=jnp.float32
    )


def own_kernel(n, vecs, me_ref, factor_ref, left_ref, scaled_ref, *refs):
    msgs, (partial_ref, kern_ref, colm_ref, rows_ref) = refs[:n], refs[n:]
    rows = msgs[0].shape[1]
    per = rows // BLK
    me = me_ref[0]
    left = jnp.concatenate([left_ref[c] for c in range(per)], axis=0)
    factors = jnp.concatenate([factor_ref[0:1, :]] * per, axis=1)
    for o in range(n):
        links = msgs[o][msgs[o].shape[0] - AUX :, :].astype(jnp.float32)[LINK_ROW : LINK_ROW + 1, :]
        for h in range(per):
            rows_ref[o * per + h : o * per + h + 1, :] = links[:, h * BLK : (h + 1) * BLK]
    table = rows_ref[...]
    lane = lax.broadcasted_iota(jnp.int32, table.shape, 1)
    for c in range(per):
        picked = jnp.sum(jnp.where(lane == me * per + c, table, 0.0), axis=1, keepdims=True)
        colm_ref[c] = jnp.broadcast_to(picked, table.shape)
    total = [jnp.zeros((vecs, BLK), jnp.float32) for _ in range(per)]
    for o in range(n):
        right = right_side(msgs[o], vecs, slice(0, rows))
        arg = lax.dot_general(left, right, (((1,), (0,)), ((), ())), preferred_element_type=jnp.float32)
        weights = jnp.exp2(arg * factors).astype(jnp.bfloat16)
        if o % 2:
            kern_ref[o // 2] = weights
        else:
            piece = scaled_ref[:, o // 2 * rows : (o // 2 + 1) * rows]
            for c in range(per):
                total[c] = total[c] + pull_tile(piece, weights[c * BLK : (c + 1) * BLK, :], colm_ref, c, o * per)
    for c in range(per):
        partial_ref[:, c * BLK : (c + 1) * BLK] = total[c]


def pull_kernel(n, partial_ref, colm_ref, kern_ref, scaled_ref, out_ref):
    rows = out_ref.shape[1]
    per = rows // BLK
    for c in range(per):
        cols = slice(c * BLK, (c + 1) * BLK)
        total = partial_ref[:, cols]
        for m in range(n // 2):
            piece = scaled_ref[:, m * rows : (m + 1) * rows]
            total = total + pull_tile(piece, kern_ref[m, cols, :], colm_ref, c, (2 * m + 1) * per)
        out_ref[:, cols] = total


def in_hbm(*arrays):
    return [pltpu.with_memory_space_constraint(a, pltpu.HBM) for a in arrays]


def add_kernel(a_ref, b_ref, out_ref):
    out_ref[...] = a_ref[...] + b_ref[...]


def per_device(n, slices, states, vectors, kernel_scale, neighbour_blocks, neighbour_count):
    coords, rows = states.shape[1], states.shape[2]
    vecs = vectors.shape[0]
    per = rows // BLK
    depth = 4 * coords + AUX
    me = lax.axis_index("traj").astype(jnp.int32).reshape(1)
    msg = pl.pallas_call(
        functools.partial(prep_kernel, n * per),
        out_shape=jax.ShapeDtypeStruct((vecs + 2 * coords + AUX, rows), jnp.bfloat16),
        in_specs=[HBM] * 4,
        out_specs=VMEM,
        scratch_shapes=[
            pltpu.SMEM(neighbour_blocks.shape, jnp.int32),
            pltpu.SMEM(neighbour_count.shape, jnp.int32),
            pltpu.VMEM(states.shape, jnp.float32),
            pltpu.SemaphoreType.DMA((4,)),
        ],
        compiler_params=PARAMS,
        name="prep",
    )(*in_hbm(neighbour_blocks, neighbour_count, states, vectors))
    factor = pl.pallas_call(
        factor_kernel,
        out_shape=jax.ShapeDtypeStruct((8, BLK), jnp.float32),
        in_specs=[SMEM],
        out_specs=VMEM,
        compiler_params=PARAMS,
        cost_estimate=pl.CostEstimate(flops=COVER, bytes_accessed=1 << 12, transcendentals=0),
        name="factor",
    )(kernel_scale)
    msgs, factor = staged_gather(msg, n, "traj", factor)
    half = n // 2
    tiles = half * per
    most = -(-neighbour_blocks.shape[1] // GROUP)
    shared = (
        jax.ShapeDtypeStruct((n * per + 1, depth, BLK), jnp.bfloat16),
        jax.ShapeDtypeStruct((n * per + 1, vecs, BLK), jnp.bfloat16),
        jax.ShapeDtypeStruct((tiles + 1, BLK, BLK), jnp.float32),
        jax.ShapeDtypeStruct((tiles + 1, vecs, BLK), jnp.float32),
    )
    lefts, lists, *state = pl.pallas_call(
        functools.partial(left_kernel, half, vecs),
        out_shape=(
            jax.ShapeDtypeStruct((tiles + 1, BLK, depth), jnp.bfloat16),
            jax.ShapeDtypeStruct((tiles + 8, BLK), jnp.int32),
            *shared,
        ),
        in_specs=[SMEM] + [VMEM] * half,
        out_specs=(VMEM,) * 6,
        compiler_params=PARAMS,
        name="left",
    )(me, *msgs[::2])
    scaled = pl.pallas_call(
        functools.partial(push_kernel, half, vecs, most),
        out_shape=(*shared, jax.ShapeDtypeStruct((vecs, half * rows), jnp.bfloat16)),
        in_specs=[SMEM] + [VMEM] * (half + 7),
        out_specs=(VMEM,) * 5,
        input_output_aliases={4 + half + i: i for i in range(4)},
        scratch_shapes=[
            pltpu.SMEM((tiles + 8, BLK), jnp.int32),
            pltpu.SMEM((tiles * most + most + BIG,), jnp.int32),
            pltpu.SemaphoreType.DMA,
        ],
        compiler_params=PARAMS,
        name="push",
    )(me, factor, lists, lefts, *msgs[1::2], *state)[4]
    across = lax.ppermute(scaled, "traj", [(i, i ^ 1) for i in range(n)])
    partial, kern, colm = pl.pallas_call(
        functools.partial(own_kernel, n, vecs),
        out_shape=(
            jax.ShapeDtypeStruct((vecs, rows), jnp.float32),
            jax.ShapeDtypeStruct((half, rows, rows), jnp.bfloat16),
            jax.ShapeDtypeStruct((per, n * per, BLK), jnp.float32),
        ),
        in_specs=[SMEM, VMEM, VMEM, VMEM] + [VMEM] * n,
        out_specs=(VMEM, VMEM, VMEM),
        scratch_shapes=[pltpu.VMEM((n * per, BLK), jnp.float32)],
        compiler_params=PARAMS,
        cost_estimate=pl.CostEstimate(flops=2 * n * rows * rows * (depth + vecs), bytes_accessed=1 << 20, transcendentals=0),
        name="own",
    )(me, factor, lefts, scaled, *msgs)
    total = pl.pallas_call(
        functools.partial(pull_kernel, n),
        out_shape=jax.ShapeDtypeStruct((vecs, rows), jnp.float32),
        in_specs=[VMEM] * 4,
        out_specs=VMEM,
        compiler_params=PARAMS,
        name="pull",
    )(partial, colm, kern, across)
    hop = 1
    while hop < slices:
        other = lax.ppermute(total, "tm", [(i, i ^ hop) for i in range(slices)])
        total = pl.pallas_call(
            add_kernel,
            out_shape=jax.ShapeDtypeStruct((vecs, rows), jnp.float32),
            in_specs=[VMEM, VMEM],
            out_specs=VMEM,
            compiler_params=PARAMS,
            name="add",
        )(total, other)
        hop *= 2
    return total


def solution(mesh):
    in_specs = (P("tm", None, "traj"), P(None, "traj"), P("tm"), P("traj", None), P("traj"))
    out_specs = P(None, "traj")
    n = mesh.shape["traj"]

    def body(*args):
        return per_device(n, mesh.shape["tm"], *args)

    return jax.shard_map(body, mesh=mesh, in_specs=in_specs, out_specs=out_specs, check_vma=False)
```

```python
import functools
import math

import jax
import jax.numpy as jnp
from jax import lax
from jax.experimental import pallas as pl
from jax.experimental.pallas import tpu as pltpu
from jax.sharding import PartitionSpec as P


BLK = 128
AUX = 8
LINK_ROW = 6
LIST_ROW = 7
GROUP = 2
COVER = 10000000
BIG = 52
SMALL = 16
ROUND = 27


VMEM = pl.BlockSpec(memory_space=pltpu.VMEM)
SMEM = pl.BlockSpec(memory_space=pltpu.SMEM)
HBM = pl.BlockSpec(memory_space=pltpu.HBM)
PARAMS = pltpu.CompilerParams(vmem_limit_bytes=16 * 1024 * 1024)


def plan(n):
    core = 2 if n % 2 == 0 else 1
    wide = 4 if n % (4 * core) == 0 else 1
    mid = n // (core * wide)
    stride = core * mid
    steps = []

    def middle(piece):
        return [(piece, k * core) for k in range(1, mid)]

    if wide == 4:
        steps += [(0, 2 * stride), (0, stride)] + middle(0) + [(2 * stride, stride)]
        steps += middle(2 * stride) + middle(stride) + middle(3 * stride)
    else:
        steps += middle(0)
    order = [0] + [piece ^ hop for piece, hop in steps]
    if core == 2:
        steps += [(piece, 1) for piece in order]
    return steps


def staged_gather(x, n, axis):
    pieces = {0: x}
    for piece, hop in plan(n):
        pieces[piece ^ hop] = lax.ppermute(pieces[piece], axis, [(d, d ^ hop) for d in range(n)])
    return [pieces[o] for o in range(n)]


def split3(value):
    first = value.astype(jnp.bfloat16)
    rest = value - first.astype(jnp.float32)
    second = rest.astype(jnp.bfloat16)
    third = (rest - second.astype(jnp.float32)).astype(jnp.bfloat16)
    return [p.astype(jnp.float32) for p in (first, second, third)]


def prep_kernel(blocks, lists_hbm, count_hbm, states_hbm, vectors_hbm, msg_ref, lists_ref, count_ref, states_ref, sems):
    vecs = vectors_hbm.shape[0]
    coords, rows = states_ref.shape[1], states_ref.shape[2]
    moves = [
        pltpu.make_async_copy(lists_hbm, lists_ref, sems.at[0]),
        pltpu.make_async_copy(count_hbm, count_ref, sems.at[1]),
        pltpu.make_async_copy(states_hbm, states_ref, sems.at[2]),
        pltpu.make_async_copy(vectors_hbm, msg_ref.at[0:vecs, :], sems.at[3]),
    ]
    for move in moves:
        move.start()
    for move in moves:
        move.wait()
    x = states_ref[0]
    hi = x.astype(jnp.bfloat16).astype(jnp.float32)
    lo = (x - hi).astype(jnp.bfloat16).astype(jnp.float32)
    whole = hi + lo
    pieces = split3(-0.5 * jnp.sum(whole * whole, axis=0, keepdims=True))
    lane = lax.broadcasted_iota(jnp.int32, (1, rows), 1)
    linked = jnp.zeros((1, rows), jnp.float32)
    listed = jnp.full((1, rows), blocks, jnp.int32)
    for h in range(rows // BLK):
        for slot in range(lists_ref.shape[1]):
            used = slot < count_ref[h]
            linked = jnp.where(lane == jnp.where(used, lists_ref[h, slot] + h * BLK, rows), 1.0, linked)
            listed = jnp.where(lane == slot + h * BLK, jnp.where(used, lists_ref[h, slot], blocks), listed)
        units = lax.shift_right_logical(count_ref[h] + (GROUP - 1), GROUP.bit_length() - 1)
        listed = jnp.where(lane == (h + 1) * BLK - 1, units, listed)
    sub = lax.broadcasted_iota(jnp.int32, (AUX, rows), 0)
    aux = jnp.where((sub >= 3) & (sub < 6), 1.0, 0.0)
    for r, piece in enumerate(pieces):
        aux = jnp.where(sub == r, piece, aux)
    aux = jnp.where(sub == LINK_ROW, linked, aux)
    aux = jnp.where(sub == LIST_ROW, listed.astype(jnp.float32), aux)
    msg_ref[vecs : vecs + coords, :] = hi.astype(jnp.bfloat16)
    msg_ref[vecs + coords : vecs + 2 * coords, :] = lo.astype(jnp.bfloat16)
    msg_ref[vecs + 2 * coords :, :] = aux.astype(jnp.bfloat16)


def factor_kernel(scale_ref, out_ref):
    out_ref[...] = (2.0 * math.log2(math.e)) / jnp.full(out_ref.shape, scale_ref[0], jnp.float32)


def right_side(msg, vecs, cols):
    feats = msg[vecs : msg.shape[0] - AUX, cols]
    return jnp.concatenate([feats, feats, msg[msg.shape[0] - AUX :, cols]], axis=0)


def stage_block(msg, vecs, base, right_ref, vec_ref):
    for h in range(msg.shape[1] // BLK):
        cols = slice(h * BLK, (h + 1) * BLK)
        right_ref[base + h] = right_side(msg, vecs, cols)
        vec_ref[base + h] = msg[0:vecs, cols]


def left_kernel(half, vecs, me_ref, *refs):
    msgs, (left_ref, lists_ref, right_ref, vec_ref, sums_ref, pushed_ref) = refs[:half], refs[half:]
    rows = msgs[0].shape[1]
    per = rows // BLK
    coords = (msgs[0].shape[0] - vecs - AUX) // 2
    blocks = 2 * half * per
    me = me_ref[0]
    sub = lax.broadcasted_iota(jnp.int32, (AUX, rows), 0)
    for m in range(half):
        hi = msgs[m][vecs : vecs + coords, :].astype(jnp.float32)
        lo = msgs[m][vecs + coords : vecs + 2 * coords, :].astype(jnp.float32)
        aux = msgs[m][vecs + 2 * coords :, :].astype(jnp.float32)
        left = jnp.where(sub < 3, 1.0, jnp.where(sub < 6, pltpu.roll(aux, 3, 0), 0.0))
        stacked = jnp.concatenate([hi, hi, lo, lo, left], axis=0).T.astype(jnp.bfloat16)
        for h in range(per):
            left_ref[m * per + h] = stacked[h * BLK : (h + 1) * BLK, :]
            row = aux[LIST_ROW : LIST_ROW + 1, h * BLK : (h + 1) * BLK]
            lists_ref[m * per + h : m * per + h + 1, :] = row.astype(jnp.int32)
        stage_block(msgs[m], vecs, (me ^ (2 * m)) * per, right_ref, vec_ref)
    lists_ref[half * per :, :] = jnp.zeros((8, BLK), jnp.int32)
    left_ref[half * per] = jnp.zeros(left_ref.shape[1:], jnp.bfloat16)
    sub = lax.broadcasted_iota(jnp.int32, right_ref.shape[1:], 0)
    right_ref[blocks] = jnp.where(sub == 4 * coords, -3.0e4, 0.0).astype(jnp.bfloat16)
    vec_ref[blocks] = jnp.zeros(vec_ref.shape[1:], jnp.bfloat16)
    sums_ref[...] = jnp.zeros(sums_ref.shape, jnp.float32)
    pushed_ref[...] = jnp.zeros(pushed_ref.shape, jnp.float32)


def push_kernel(half, vecs, most, me_ref, factor_ref, lists_ref, left_ref, *refs):
    msgs, refs = refs[:half], refs[half + 4 :]
    right_ref, vec_ref, sums_ref, pushed_ref, scaled_ref, list_ref, unit_ref, sem = refs
    per = msgs[0].shape[1] // BLK
    tiles = half * per
    move = pltpu.make_async_copy(lists_ref, list_ref, sem)
    move.start()
    me = me_ref[0]
    for m in range(half):
        stage_block(msgs[m], vecs, (me ^ (2 * m + 1)) * per, right_ref, vec_ref)
    factors = jnp.concatenate([factor_ref[0:1, :]] * GROUP, axis=1)
    move.wait()
    start = 0
    for r in range(tiles):
        for k in range(most):
            unit_ref[start + k] = r * BLK + k * GROUP
        start = start + list_ref[r, BLK - 1]
    for k in range(BIG):
        unit_ref[start + k] = tiles * BLK

    def visit(code):
        r = lax.shift_right_logical(code, 7)
        k = lax.bitwise_and(code, BLK - 1)
        ids = [list_ref[r, k + q] for q in range(GROUP)]
        right = jnp.concatenate([right_ref[b] for b in ids], axis=1)
        arg = lax.dot_general(left_ref[r], right, (((1,), (0,)), ((), ())), preferred_element_type=jnp.float32)
        kernel = jnp.exp2(arg * factors)
        weights = kernel.astype(jnp.bfloat16)
        total = kernel[:, 0:BLK]
        for q in range(1, GROUP):
            total = total + kernel[:, q * BLK : (q + 1) * BLK]
        vec = jnp.concatenate([vec_ref[b] for b in ids], axis=1)
        push = lax.dot_general(vec, weights, (((1,), (1,)), ((), ())), preferred_element_type=jnp.float32)
        sums_ref[r] = sums_ref[r] + total
        pushed_ref[r] = pushed_ref[r] + push

    def big_step(t, carry):
        for g in range(BIG):
            visit(unit_ref[t * BIG + g])
        return carry

    def small_step(t, first):
        for g in range(SMALL):
            visit(unit_ref[first + t * SMALL + g])
        return first

    bigs = lax.div(start + ROUND, BIG)
    rest = jnp.maximum(start - bigs * BIG, 0)
    lax.fori_loop(0, bigs, big_step, 0)
    lax.fori_loop(0, lax.div(rest + (SMALL - 1), SMALL), small_step, bigs * BIG)
    for r in range(tiles):
        row_sum = jnp.sum(sums_ref[r].T, axis=0, keepdims=True)
        scaled_ref[:, r * BLK : (r + 1) * BLK] = (pushed_ref[r] / (row_sum * row_sum)).astype(jnp.bfloat16)


def pull_tile(piece, kernel, colm_ref, c, block):
    parts = []
    for h in range(piece.shape[1] // BLK):
        m = colm_ref[c, block + h : block + h + 1, :]
        part = piece[:, h * BLK : (h + 1) * BLK].astype(jnp.float32)
        parts.append(jnp.where(m > 0.5, part, 0.0).astype(jnp.bfloat16))
    return lax.dot_general(
        jnp.concatenate(parts, axis=1), kernel, (((1,), (1,)), ((), ())), preferred_element_type=jnp.float32
    )


def own_kernel(n, vecs, me_ref, factor_ref, left_ref, scaled_ref, *refs):
    msgs, (partial_ref, kern_ref, colm_ref, rows_ref) = refs[:n], refs[n:]
    rows = msgs[0].shape[1]
    per = rows // BLK
    me = me_ref[0]
    left = jnp.concatenate([left_ref[c] for c in range(per)], axis=0)
    factors = jnp.concatenate([factor_ref[0:1, :]] * per, axis=1)
    for o in range(n):
        links = msgs[o][msgs[o].shape[0] - AUX :, :].astype(jnp.float32)[LINK_ROW : LINK_ROW + 1, :]
        for h in range(per):
            rows_ref[o * per + h : o * per + h + 1, :] = links[:, h * BLK : (h + 1) * BLK]
    table = rows_ref[...]
    lane = lax.broadcasted_iota(jnp.int32, table.shape, 1)
    for c in range(per):
        picked = jnp.sum(jnp.where(lane == me * per + c, table, 0.0), axis=1, keepdims=True)
        colm_ref[c] = jnp.broadcast_to(picked, table.shape)
    total = [jnp.zeros((vecs, BLK), jnp.float32) for _ in range(per)]
    for o in range(n):
        right = right_side(msgs[o], vecs, slice(0, rows))
        arg = lax.dot_general(left, right, (((1,), (0,)), ((), ())), preferred_element_type=jnp.float32)
        weights = jnp.exp2(arg * factors).astype(jnp.bfloat16)
        if o % 2:
            kern_ref[o // 2] = weights
        else:
            piece = scaled_ref[:, o // 2 * rows : (o // 2 + 1) * rows]
            for c in range(per):
                total[c] = total[c] + pull_tile(piece, weights[c * BLK : (c + 1) * BLK, :], colm_ref, c, o * per)
    for c in range(per):
        partial_ref[:, c * BLK : (c + 1) * BLK] = total[c]


def pull_kernel(n, partial_ref, colm_ref, kern_ref, scaled_ref, out_ref):
    rows = out_ref.shape[1]
    per = rows // BLK
    for c in range(per):
        cols = slice(c * BLK, (c + 1) * BLK)
        total = partial_ref[:, cols]
        for m in range(n // 2):
            piece = scaled_ref[:, m * rows : (m + 1) * rows]
            total = total + pull_tile(piece, kern_ref[m, cols, :], colm_ref, c, (2 * m + 1) * per)
        out_ref[:, cols] = total


def in_hbm(*arrays):
    return [pltpu.with_memory_space_constraint(a, pltpu.HBM) for a in arrays]


def add_kernel(a_ref, b_ref, out_ref):
    out_ref[...] = a_ref[...] + b_ref[...]


def per_device(n, slices, states, vectors, kernel_scale, neighbour_blocks, neighbour_count):
    coords, rows = states.shape[1], states.shape[2]
    vecs = vectors.shape[0]
    per = rows // BLK
    depth = 4 * coords + AUX
    me = lax.axis_index("traj").astype(jnp.int32).reshape(1)
    msg = pl.pallas_call(
        functools.partial(prep_kernel, n * per),
        out_shape=jax.ShapeDtypeStruct((vecs + 2 * coords + AUX, rows), jnp.bfloat16),
        in_specs=[HBM] * 4,
        out_specs=VMEM,
        scratch_shapes=[
            pltpu.SMEM(neighbour_blocks.shape, jnp.int32),
            pltpu.SMEM(neighbour_count.shape, jnp.int32),
            pltpu.VMEM(states.shape, jnp.float32),
            pltpu.SemaphoreType.DMA((4,)),
        ],
        compiler_params=PARAMS,
        name="prep",
    )(*in_hbm(neighbour_blocks, neighbour_count, states, vectors))
    factor = pl.pallas_call(
        factor_kernel,
        out_shape=jax.ShapeDtypeStruct((8, BLK), jnp.float32),
        in_specs=[SMEM],
        out_specs=VMEM,
        compiler_params=PARAMS,
        cost_estimate=pl.CostEstimate(flops=COVER, bytes_accessed=1 << 12, transcendentals=0),
        name="factor",
    )(kernel_scale)
    msgs = staged_gather(msg, n, "traj")
    half = n // 2
    tiles = half * per
    most = -(-neighbour_blocks.shape[1] // GROUP)
    shared = (
        jax.ShapeDtypeStruct((n * per + 1, depth, BLK), jnp.bfloat16),
        jax.ShapeDtypeStruct((n * per + 1, vecs, BLK), jnp.bfloat16),
        jax.ShapeDtypeStruct((tiles + 1, BLK, BLK), jnp.float32),
        jax.ShapeDtypeStruct((tiles + 1, vecs, BLK), jnp.float32),
    )
    lefts, lists, *state = pl.pallas_call(
        functools.partial(left_kernel, half, vecs),
        out_shape=(
            jax.ShapeDtypeStruct((tiles + 1, BLK, depth), jnp.bfloat16),
            jax.ShapeDtypeStruct((tiles + 8, BLK), jnp.int32),
            *shared,
        ),
        in_specs=[SMEM] + [VMEM] * half,
        out_specs=(VMEM,) * 6,
        compiler_params=PARAMS,
        name="left",
    )(me, *msgs[::2])
    scaled = pl.pallas_call(
        functools.partial(push_kernel, half, vecs, most),
        out_shape=(*shared, jax.ShapeDtypeStruct((vecs, half * rows), jnp.bfloat16)),
        in_specs=[SMEM] + [VMEM] * (half + 7),
        out_specs=(VMEM,) * 5,
        input_output_aliases={4 + half + i: i for i in range(4)},
        scratch_shapes=[
            pltpu.SMEM((tiles + 8, BLK), jnp.int32),
            pltpu.SMEM((tiles * most + most + BIG,), jnp.int32),
            pltpu.SemaphoreType.DMA,
        ],
        compiler_params=PARAMS,
        name="push",
    )(me, factor, lists, lefts, *msgs[1::2], *state)[4]
    across = lax.ppermute(scaled, "traj", [(i, i ^ 1) for i in range(n)])
    partial, kern, colm = pl.pallas_call(
        functools.partial(own_kernel, n, vecs),
        out_shape=(
            jax.ShapeDtypeStruct((vecs, rows), jnp.float32),
            jax.ShapeDtypeStruct((half, rows, rows), jnp.bfloat16),
            jax.ShapeDtypeStruct((per, n * per, BLK), jnp.float32),
        ),
        in_specs=[SMEM, VMEM, VMEM, VMEM] + [VMEM] * n,
        out_specs=(VMEM, VMEM, VMEM),
        scratch_shapes=[pltpu.VMEM((n * per, BLK), jnp.float32)],
        compiler_params=PARAMS,
        cost_estimate=pl.CostEstimate(flops=2 * n * rows * rows * (depth + vecs), bytes_accessed=1 << 20, transcendentals=0),
        name="own",
    )(me, factor, lefts, scaled, *msgs)
    total = pl.pallas_call(
        functools.partial(pull_kernel, n),
        out_shape=jax.ShapeDtypeStruct((vecs, rows), jnp.float32),
        in_specs=[VMEM] * 4,
        out_specs=VMEM,
        compiler_params=PARAMS,
        name="pull",
    )(partial, colm, kern, across)
    hop = 1
    while hop < slices:
        other = lax.ppermute(total, "tm", [(i, i ^ hop) for i in range(slices)])
        total = pl.pallas_call(
            add_kernel,
            out_shape=jax.ShapeDtypeStruct((vecs, rows), jnp.float32),
            in_specs=[VMEM, VMEM],
            out_specs=VMEM,
            compiler_params=PARAMS,
            name="add",
        )(total, other)
        hop *= 2
    return total


def solution(mesh):
    in_specs = (P("tm", None, "traj"), P(None, "traj"), P("tm"), P("traj", None), P("traj"))
    out_specs = P(None, "traj")
    n = mesh.shape["traj"]

    def body(*args):
        return per_device(n, mesh.shape["tm"], *args)

    return jax.shard_map(body, mesh=mesh, in_specs=in_specs, out_specs=out_specs, check_vma=False)
```
